32 devices in a mesh: head: 4 (over z), pts: 8 (over y, x, core).
Axes of the slice: x: 2, y: 2, z: 4, core: 2. Of those that a mesh axis runs over, the one named last changes fastest.
Arguments:
- layer_inputs_trainorder: bfloat16 [196608, 256], P(('head', 'pts')), may hold values from -6 to 6
- inference_placement: int32 [196608], P(('head', 'pts')), may hold values from 0 to 196607, as said below
- initial_layernorm_gain: float32 [256], replicated, may hold values from 0.1 to 1.9
- initial_layernorm_offset: float32 [256], replicated, may hold values from -2 to 2
- attribute_projection: bfloat16 [256, 256], replicated, may hold values from -0.375 to 0.375
- assignment_feeder_projection: bfloat16 [256, 256], replicated, may hold values from -0.375 to 0.375
- partition_projection: bfloat16 [16, 32], replicated, may hold values from -1.5 to 1.5
- partition_offset: float32 [32], replicated, may hold values from -4 to 4
- softmax_sharpness: float32 [16], P('head'), may hold values from 0.03 to 1
- partition_question_map: float32 [16, 16], replicated, may hold values from -1.5 to 1.5
- partition_lookup_map: float32 [16, 16], replicated, may hold values from -1.5 to 1.5
- partition_content_map: float32 [16, 16], replicated, may hold values from -1.5 to 1.5
- emitted_projection: bfloat16 [256, 256], replicated, may hold values from -0.375 to 0.375
- emitted_offset: float32 [256], replicated, may hold values from -2 to 2
- latter_layernorm_gain: float32 [256], replicated, may hold values from 0.1 to 1.9
- latter_layernorm_offset: float32 [256], replicated, may hold values from -2 to 2
- perceptron_entry_map: bfloat16 [256, 1024], replicated, may hold values from -0.375 to 0.375
- perceptron_entry_offset: float32 [1024], replicated, may hold values from -2 to 2
- perceptron_exit_map: bfloat16 [1024, 256], replicated, may hold values from -0.1875 to 0.1875
- perceptron_exit_offset: float32 [256], replicated, may hold values from -2 to 2
Outputs:
- served: bfloat16 [8, 24576, 256], P('pts', 'head')
The draws below stay inside these ranges and needn't reach their ends.
Inputs may be any that keep to these rules, and one draw needn't show every extreme that they name: inference_placement is a permutation of all points; of the 6144 points of each aligned block of the training order, exactly 192 go to each aligned block of 6144 serving positions.
All inputs are finite; a program needn't handle non-finite values.
Results may differ from the reference program's by a relative error of at most 0.0035.
The reference program's roundings to bfloat16 on the way count: a program that leaves them out, or rounds other values in their place, can miss the bound.
Values may be sent and summed in bfloat16 or wider, within the bound.
A program may use at most 128 MiB of HBM per device.

```python
import math
import jax
import jax.numpy as jnp
from jax import lax

ATTENDER_TOTAL = 16
DH = 16
M = 32
FF = 1024
PTS_DEV = 6144
MODEL_CHANNELS = 256
SERVE = 24576
POINTS = 196608
N_PTS = 8


def draw_inference_placement(key, part):
    blocks = POINTS // PTS_DEV
    per_pair = PTS_DEV // blocks
    first_keys = jax.random.split(jax.random.fold_in(key, 11), blocks)
    second_keys = jax.random.split(jax.random.fold_in(key, 12), blocks)
    within = jax.vmap(lambda single: jax.random.permutation(single, PTS_DEV))(first_keys).astype(jnp.int32)
    arrival = jax.vmap(lambda single: jax.random.permutation(single, PTS_DEV))(second_keys).astype(jnp.int32)
    target = within // per_pair
    ranks_in = within % per_pair
    source_ids = jnp.arange(blocks, dtype=jnp.int32)[:, None]
    slot_ids = source_ids * per_pair + ranks_in
    positions = target * PTS_DEV + arrival[target, slot_ids]
    return positions.reshape(-1).astype(jnp.int32)


def level_of(key, shape, cuts, smallest, high):
    loudness, own = 1.0, jax.random.fold_in(key, 6)
    for axis_at, parts in cuts:
        steps = jnp.exp(jax.random.uniform(jax.random.fold_in(own, axis_at), (parts,), jnp.float32, smallest / len(cuts), high / len(cuts)))
        loudness = loudness * jnp.repeat(steps, shape[axis_at] // parts).reshape([-1 if axis == axis_at else 1 for axis in range(len(shape))])
    return loudness


def bell_draw(stream_key, shape, deviation, bound, cuts=(), held_as=jnp.bfloat16):
    loudness = level_of(stream_key, shape, cuts, -0.22, 0.18) if cuts else 1.0
    result = jax.random.normal(stream_key, shape, jnp.float32) * deviation * loudness
    return jnp.minimum(jnp.maximum(result, -bound), bound).astype(held_as)


def setup_inputs(seed: int = 0) -> dict:
    key_of = jax.random.split(jax.random.key(seed), 21)
    return {
        "layer_inputs_trainorder": bell_draw(key_of[0], (POINTS, MODEL_CHANNELS), 1.0, 6.0, ((0, 32),)),
        "inference_placement": draw_inference_placement(jax.random.fold_in(key_of[20], 71), 0),
        "initial_layernorm_gain": jnp.clip(1.0 + 0.18 * jax.random.normal(key_of[2], (MODEL_CHANNELS,), jnp.float32), 0.1, 1.9),
        "initial_layernorm_offset": bell_draw(key_of[3], (MODEL_CHANNELS,), 0.3, 2.0, (), jnp.float32),
        "attribute_projection": bell_draw(key_of[4], (MODEL_CHANNELS, MODEL_CHANNELS), MODEL_CHANNELS ** -0.5, 0.375),
        "assignment_feeder_projection": bell_draw(key_of[5], (MODEL_CHANNELS, MODEL_CHANNELS), MODEL_CHANNELS ** -0.5, 0.375),
        "partition_projection": bell_draw(key_of[6], (DH, M), DH ** -0.5, 1.5),
        "partition_offset": bell_draw(key_of[7], (M,), 1.0, 4.0, (), jnp.float32),
        "softmax_sharpness": jnp.clip(jnp.exp(math.log(1.0) - 3.506558 * jax.random.uniform(key_of[8], (ATTENDER_TOTAL,), jnp.float32) ** level_of(key_of[8], (ATTENDER_TOTAL,), ((0, 4),), -0.2, 0.2)), 0.03, 1.0),
        "partition_question_map": bell_draw(key_of[9], (DH, DH), DH ** -0.5, 1.5, (), jnp.float32),
        "partition_lookup_map": bell_draw(key_of[10], (DH, DH), DH ** -0.5, 1.5, (), jnp.float32),
        "partition_content_map": bell_draw(key_of[11], (DH, DH), DH ** -0.5, 1.5, (), jnp.float32),
        "emitted_projection": bell_draw(key_of[12], (MODEL_CHANNELS, MODEL_CHANNELS), MODEL_CHANNELS ** -0.5, 0.375),
        "emitted_offset": bell_draw(key_of[13], (MODEL_CHANNELS,), 0.3, 2.0, (), jnp.float32),
        "latter_layernorm_gain": jnp.clip(1.0 + 0.18 * jax.random.normal(key_of[14], (MODEL_CHANNELS,), jnp.float32), 0.1, 1.9),
        "latter_layernorm_offset": bell_draw(key_of[15], (MODEL_CHANNELS,), 0.3, 2.0, (), jnp.float32),
        "perceptron_entry_map": bell_draw(key_of[16], (MODEL_CHANNELS, FF), MODEL_CHANNELS ** -0.5, 0.375),
        "perceptron_entry_offset": bell_draw(key_of[17], (FF,), 0.3, 2.0, (), jnp.float32),
        "perceptron_exit_map": bell_draw(key_of[18], (FF, MODEL_CHANNELS), FF ** -0.5, 0.1875),
        "perceptron_exit_offset": bell_draw(key_of[19], (MODEL_CHANNELS,), 0.3, 2.0, (), jnp.float32),
    }


def layer_norm(row_block, gain_vec, bias_vec):
    row_mean = lax.optimization_barrier(jnp.mean(row_block, axis=-1, keepdims=True))
    centred = row_block - row_mean
    spread = lax.optimization_barrier(jnp.mean(centred * centred, axis=-1, keepdims=True))
    return centred * lax.rsqrt(spread + 1e-05) * gain_vec + bias_vec

def truncated_coefficients(value):
    return lax.optimization_barrier(value.astype(jnp.bfloat16)).astype(jnp.float32)

def partition_share_entries(standardized_entries, assignment_feeder_projection, partition_projection, partition_offset, softmax_sharpness):
    middle = truncated_coefficients(jnp.dot(standardized_entries, assignment_feeder_projection, preferred_element_type=jnp.float32)).reshape(-1, ATTENDER_TOTAL, DH)
    partition_scores_raw = jnp.einsum('rhd,dm->rhm', middle, partition_projection.astype(jnp.float32))
    partition_scores_raw = (partition_scores_raw + partition_offset) / softmax_sharpness[:, None]
    return jax.nn.softmax(partition_scores_raw, axis=-1)

def reference(layer_inputs_trainorder, inference_placement, initial_layernorm_gain, initial_layernorm_offset, attribute_projection, assignment_feeder_projection, partition_projection, partition_offset, softmax_sharpness, partition_question_map, partition_lookup_map, partition_content_map, emitted_projection, emitted_offset, latter_layernorm_gain, latter_layernorm_offset, perceptron_entry_map, perceptron_entry_offset, perceptron_exit_map, perceptron_exit_offset):
    block_count = POINTS // PTS_DEV
    row_blocks = layer_inputs_trainorder.reshape(block_count, PTS_DEV, MODEL_CHANNELS)

    def gather_sums(running_state, row_block):
        standardized_entries = layer_norm(row_block.astype(jnp.float32), initial_layernorm_gain, initial_layernorm_offset).astype(jnp.bfloat16)
        slice_feature_rows = truncated_coefficients(jnp.dot(standardized_entries, attribute_projection, preferred_element_type=jnp.float32)).reshape(-1, ATTENDER_TOTAL, DH)
        coefficient_array = partition_share_entries(standardized_entries, assignment_feeder_projection, partition_projection, partition_offset, softmax_sharpness)
        coefficients_halfprecision = truncated_coefficients(coefficient_array)
        return ((running_state[0] + lax.optimization_barrier(jnp.sum(coefficient_array, axis=0)), running_state[1] + jnp.einsum('qct,qcv->ctv', coefficients_halfprecision, slice_feature_rows)), None)
    start = (jnp.zeros((ATTENDER_TOTAL, M), jnp.float32), jnp.zeros((ATTENDER_TOTAL, M, DH), jnp.float32))
    (totals, numerator), unused = lax.scan(gather_sums, start, row_blocks)
    slice_token = numerator / (totals + 1e-05)[:, :, None]
    highest_mode = lax.Precision.HIGHEST
    query_rows = jnp.einsum('izn,nu->izu', slice_token, partition_question_map, precision=highest_mode)
    key_vectors = jnp.einsum('izn,nu->izu', slice_token, partition_lookup_map, precision=highest_mode)
    value_rows = jnp.einsum('izn,nu->izu', slice_token, partition_content_map, precision=highest_mode)
    score_scale = 1.0 / math.sqrt(DH)
    scores = jnp.einsum('hme,hne->hmn', query_rows, key_vectors, precision=highest_mode) * score_scale
    attention = jax.nn.softmax(scores, axis=-1)
    slice_output = truncated_coefficients(jnp.einsum('hmn,hne->hme', attention, value_rows, precision=highest_mode))
    inverse = jnp.argsort(inference_placement).astype(jnp.int32).reshape(block_count, PTS_DEV)

    def serve_block(serve_index):
        row_block = jnp.take(layer_inputs_trainorder, serve_index, axis=0)
        standardized_entries = layer_norm(row_block.astype(jnp.float32), initial_layernorm_gain, initial_layernorm_offset).astype(jnp.bfloat16)
        coefficients_halfprecision = truncated_coefficients(partition_share_entries(standardized_entries, assignment_feeder_projection, partition_projection, partition_offset, softmax_sharpness))
        blended_rows = jnp.einsum('fny,nyp->fnp', coefficients_halfprecision, slice_output).astype(jnp.bfloat16).reshape(-1, MODEL_CHANNELS)
        hidden = row_block.astype(jnp.float32) + jnp.dot(blended_rows, emitted_projection, preferred_element_type=jnp.float32) + emitted_offset
        normed_two = layer_norm(hidden, latter_layernorm_gain, latter_layernorm_offset).astype(jnp.bfloat16)
        inner_act = jax.nn.gelu(jnp.dot(normed_two, perceptron_entry_map, preferred_element_type=jnp.float32) + perceptron_entry_offset, approximate=False).astype(jnp.bfloat16)
        return (hidden + jnp.dot(inner_act, perceptron_exit_map, preferred_element_type=jnp.float32) + perceptron_exit_offset).astype(jnp.bfloat16)
    served = lax.map(serve_block, inverse)
    return served.reshape(N_PTS, SERVE, MODEL_CHANNELS)
```

```python
import functools
import math

import jax
import jax.numpy as jnp
from jax import lax
from jax.experimental import pallas as pl
from jax.experimental.pallas import tpu as pltpu
from jax.sharding import PartitionSpec as P

DH = 16
TILE = 512
F32 = jnp.float32
BF16 = jnp.bfloat16
HIGHEST = lax.Precision.HIGHEST
LOG2E = math.log2(math.e)
NT = (((1,), (1,)), ((), ()))


def norm_rows(rows, gain, bias):
    mean = jnp.mean(rows, axis=-1, keepdims=True)
    centred = rows - mean
    spread = jnp.mean(centred * centred, axis=-1, keepdims=True)
    return (centred * lax.rsqrt(spread + 1e-05) * gain + bias).astype(BF16)


def slice_weights(feeder_t, expand, offset, scale, slices):
    raw = jnp.dot(expand, feeder_t, preferred_element_type=F32)
    logit = (raw + offset) * scale
    lanes = logit.shape[1]
    logit = logit.reshape(-1, slices, lanes)
    powers = jnp.exp2(logit - jnp.max(logit, axis=1, keepdims=True))
    share = powers * (1.0 / jnp.sum(powers, axis=1, keepdims=True))
    return share.reshape(-1, lanes)


def same_head(shape, row_size, column_size):
    row_head = lax.broadcasted_iota(jnp.int32, shape, 0) // row_size
    column_head = lax.broadcasted_iota(jnp.int32, shape, 1) // column_size
    return row_head == column_head


def sums_kernel(
    slices, x_ref, gain_ref, bias_ref, w_ref, expand_ref, offset_ref, scale_ref,
    out_ref, numer, total,
):
    step = pl.program_id(0)
    width = x_ref.shape[1]

    @pl.when(step == 0)
    def _():
        numer[...] = jnp.zeros_like(numer)
        total[...] = jnp.zeros_like(total)

    normed = norm_rows(x_ref[...].astype(F32), gain_ref[...], bias_ref[...])
    both = lax.dot_general(w_ref[...], normed, NT, preferred_element_type=F32).astype(BF16)
    share = slice_weights(
        both[width:], expand_ref[...], offset_ref[...], scale_ref[...], slices
    )
    numer[...] += lax.dot_general(
        both[:width], share.astype(BF16), NT, preferred_element_type=F32
    )
    lanes = total.shape[1]
    part = share[:, :lanes]
    for at in range(lanes, share.shape[1], lanes):
        part += share[:, at : at + lanes]
    total[...] += part

    @pl.when(step == pl.num_programs(0) - 1)
    def _():
        kept = jnp.where(same_head(numer.shape, DH, slices), numer[...], 0.0)
        out_ref[:DH] = jnp.sum(kept.reshape(-1, DH, kept.shape[1]), axis=0)
        out_ref[DH:] = lax.dot_general(
            jnp.ones((8, lanes), F32), total[...], NT, precision=HIGHEST,
            preferred_element_type=F32,
        )


def exact_gelu(h):
    size = jnp.abs(h)
    t = 1.0 / (1.0 + (0.3275911 / math.sqrt(2.0)) * size)
    poly = (0.5 * 1.061405429) * t + (0.5 * -1.453152027)
    poly = poly * t + (0.5 * 1.421413741)
    poly = poly * t + (0.5 * -0.284496736)
    poly = poly * t + (0.5 * 0.254829592)
    tail = (poly * t) * jnp.exp2((h * h) * (-0.5 * LOG2E))
    return jnp.maximum(h, 0.0) - size * tail


def rows_kernel(
    slices, x_ref, sums_ref, qkv_ref, gain_ref, bias_ref, w_ref, expand_ref, offset_ref,
    scale_ref, emit_ref, emit_bias_ref, gain2_ref, bias2_ref, entry_ref, entry_bias_ref,
    exit_ref, exit_bias_ref, out_ref, blend,
):
    @pl.when(pl.program_id(0) == 0)
    def _():
        stok = sums_ref[:DH] / (sums_ref[DH : DH + 1] + 1e-05)
        qkv = jnp.dot(qkv_ref[...], stok, precision=HIGHEST, preferred_element_type=F32)
        query, key, value = qkv[:DH], qkv[DH : 2 * DH], qkv[2 * DH :]
        scores = jnp.dot(key.T, query, precision=HIGHEST, preferred_element_type=F32)
        scores = scores * (1.0 / math.sqrt(DH))
        mask = same_head(scores.shape, slices, slices)
        scores = jnp.where(mask, scores, -jnp.inf)
        powers = jnp.exp(scores - jnp.max(scores, axis=0, keepdims=True))
        attention = powers / jnp.sum(powers, axis=0, keepdims=True)
        sout = jnp.dot(value, attention, precision=HIGHEST, preferred_element_type=F32)
        spread = jnp.concatenate([sout] * (blend.shape[0] // DH), axis=0)
        blend[...] = jnp.where(same_head(blend.shape, DH, slices), spread, 0.0).astype(BF16)

    x = x_ref[...].astype(F32)
    normed = norm_rows(x, gain_ref[...], bias_ref[...])
    feeder = lax.dot_general(w_ref[...], normed, NT, preferred_element_type=F32).astype(BF16)
    share = slice_weights(feeder, expand_ref[...], offset_ref[...], scale_ref[...], slices)
    mixed = jnp.dot(blend[...], share.astype(BF16), preferred_element_type=F32)
    y = (
        x
        + jnp.dot(mixed.T.astype(BF16), emit_ref[...], preferred_element_type=F32)
        + emit_bias_ref[...]
    )
    z = norm_rows(y, gain2_ref[...], bias2_ref[...])
    result = y + exit_bias_ref[...]
    chunk = x_ref.shape[1]
    for at in range(0, entry_ref.shape[1], chunk):
        h = jnp.dot(z, entry_ref[:, at : at + chunk], preferred_element_type=F32)
        g = exact_gelu(h + entry_bias_ref[:, at : at + chunk]).astype(BF16)
        result += jnp.dot(g, exit_ref[at : at + chunk], preferred_element_type=F32)
    out_ref[...] = result.astype(BF16)


def whole(array):
    return pl.BlockSpec(array.shape, lambda i: (0,) * array.ndim)


def body(
    layer_inputs_trainorder,
    inference_placement,
    initial_layernorm_gain,
    initial_layernorm_offset,
    attribute_projection,
    assignment_feeder_projection,
    partition_projection,
    partition_offset,
    softmax_sharpness,
    partition_question_map,
    partition_lookup_map,
    partition_content_map,
    emitted_projection,
    emitted_offset,
    latter_layernorm_gain,
    latter_layernorm_offset,
    perceptron_entry_map,
    perceptron_entry_offset,
    perceptron_exit_map,
    perceptron_exit_offset,
):
    groups = lax.axis_size("head")
    shards = lax.axis_size("pts")
    devices = groups * shards
    local_rows, width = layer_inputs_trainorder.shape
    per_pair = local_rows // devices
    own_heads = softmax_sharpness.shape[0]
    heads = own_heads * groups
    slices = partition_projection.shape[1]
    columns = heads * slices
    tile = math.gcd(TILE, local_rows)

    dest_block = inference_placement // local_rows
    target = dest_block % groups * shards + dest_block // groups
    send_key = target * local_rows + inference_placement % local_rows
    counting = jnp.arange(local_rows, dtype=jnp.int32)
    send_key, ordering = lax.sort((send_key, counting), num_keys=1)
    spots = (send_key % local_rows).astype(F32).reshape(devices, per_pair)
    small = jnp.concatenate(
        [spots, jnp.broadcast_to(softmax_sharpness, (devices, own_heads))], axis=1
    )
    small = lax.all_to_all(small, ("head", "pts"), split_axis=0, concat_axis=0, tiled=True)
    sharpness = small.reshape(groups, shards, -1)[:, 0, per_pair:].reshape(heads)
    arrived_spots = small[:, :per_pair].reshape(local_rows).astype(jnp.int32)
    arrived = lax.all_to_all(
        layer_inputs_trainorder[ordering], ("head", "pts"), split_axis=0, concat_axis=0,
        tiled=True,
    )
    _, placed = lax.sort((arrived_spots, counting), num_keys=1)

    gain = initial_layernorm_gain[None]
    bias = initial_layernorm_offset[None]
    feeder_t = assignment_feeder_projection.T
    both_t = jnp.concatenate([attribute_projection.T, feeder_t], axis=0)
    expand = (
        jnp.eye(heads, dtype=BF16)[:, None, :, None] * partition_projection.T[None, :, None, :]
    ).reshape(columns, width)
    offset = jnp.tile(partition_offset, heads)[:, None]
    scale = jnp.repeat(LOG2E / sharpness, slices)[:, None]

    row_spec = pl.BlockSpec((tile, width), lambda i: (i, 0))
    operands = (gain, bias, both_t, expand, offset, scale)
    sums = pl.pallas_call(
        functools.partial(sums_kernel, slices),
        grid=(local_rows // tile,),
        in_specs=[row_spec] + [whole(a) for a in operands],
        out_specs=pl.BlockSpec((DH + 8, columns), lambda i: (0, 0)),
        out_shape=jax.ShapeDtypeStruct((DH + 8, columns), F32),
        scratch_shapes=[pltpu.VMEM((width, columns), F32), pltpu.VMEM((columns, 128), F32)],
        compiler_params=pltpu.CompilerParams(dimension_semantics=("arbitrary",)),
        cost_estimate=pl.CostEstimate(
            flops=local_rows * width * columns * 8, bytes_accessed=local_rows * width * 16,
            transcendentals=local_rows * columns,
        ),
    )(layer_inputs_trainorder, *operands)
    sums = lax.psum(sums, ("head", "pts"))

    qkv = jnp.concatenate(
        [partition_question_map.T, partition_lookup_map.T, partition_content_map.T], axis=0
    )
    operands = (
        sums, qkv, gain, bias, feeder_t, expand, offset, scale, emitted_projection,
        emitted_offset[None], latter_layernorm_gain[None], latter_layernorm_offset[None],
        perceptron_entry_map, perceptron_entry_offset[None], perceptron_exit_map,
        perceptron_exit_offset[None],
    )
    result = pl.pallas_call(
        functools.partial(rows_kernel, slices),
        grid=(local_rows // tile,),
        in_specs=[row_spec] + [whole(a) for a in operands],
        out_specs=row_spec,
        out_shape=jax.ShapeDtypeStruct((local_rows, width), BF16),
        scratch_shapes=[pltpu.VMEM((width, columns), BF16)],
        compiler_params=pltpu.CompilerParams(dimension_semantics=("arbitrary",)),
        cost_estimate=pl.CostEstimate(
            flops=local_rows * width * columns * 16, bytes_accessed=local_rows * width * 16,
            transcendentals=local_rows * columns * 4,
        ),
    )(arrived, *operands)
    return result[placed][None]


def solution(mesh):
    placed = (
        P(("head", "pts"), None),
        P(("head", "pts")),
        P(),
        P(),
        P(),
        P(),
        P(),
        P(),
        P("head"),
        P(),
        P(),
        P(),
        P(),
        P(),
        P(),
        P(),
        P(),
        P(),
        P(),
        P(),
    )
    return jax.shard_map(
        body, mesh=mesh, in_specs=placed, out_specs=P("pts", "head", None), check_vma=False
    )
```

```python
import functools
import math

import jax
import jax.numpy as jnp
from jax import lax
from jax.experimental import pallas as pl
from jax.experimental.pallas import tpu as pltpu
from jax.sharding import PartitionSpec as P

DH = 16
TILE = 512
CHUNKS = 3
F32 = jnp.float32
BF16 = jnp.bfloat16
HIGHEST = lax.Precision.HIGHEST
LOG2E = math.log2(math.e)
NT = (((1,), (1,)), ((), ()))


def norm_rows(rows, gain, bias):
    mean = jnp.mean(rows, axis=-1, keepdims=True)
    centred = rows - mean
    spread = jnp.mean(centred * centred, axis=-1, keepdims=True)
    return (centred * lax.rsqrt(spread + 1e-05) * gain + bias).astype(BF16)


def slice_weights(feeder_t, expand, offset, scale, slices):
    raw = jnp.dot(expand, feeder_t, preferred_element_type=F32)
    logit = (raw + offset) * scale
    lanes = logit.shape[1]
    logit = logit.reshape(-1, slices, lanes)
    powers = jnp.exp2(logit - jnp.max(logit, axis=1, keepdims=True))
    share = powers * (1.0 / jnp.sum(powers, axis=1, keepdims=True))
    return share.reshape(-1, lanes)


def same_head(shape, row_size, column_size):
    row_head = lax.broadcasted_iota(jnp.int32, shape, 0) // row_size
    column_head = lax.broadcasted_iota(jnp.int32, shape, 1) // column_size
    return row_head == column_head


def sums_kernel(
    slices, x_ref, gain_ref, bias_ref, attribute_ref, feeder_ref, project_ref, offset_row_ref,
    sharp_row_ref, out_ref, w_ref, expand_ref, offset_ref, scale_ref, numer, total,
):
    step = pl.program_id(0)
    width = x_ref.shape[1]

    @pl.when(step == 0)
    def _():
        numer[...] = jnp.zeros_like(numer)
        total[...] = jnp.zeros_like(total)
        w_ref[:width] = attribute_ref[...].astype(F32).T.astype(BF16)
        w_ref[width:] = feeder_ref[...].astype(F32).T.astype(BF16)
        columns, heads = offset_ref.shape[0], sharp_row_ref.shape[1]
        stacked = jnp.concatenate([project_ref[...].astype(F32).T] * heads, axis=0)
        lane = lax.broadcasted_iota(jnp.int32, (DH, width), 1) % DH
        pick = (lane == lax.broadcasted_iota(jnp.int32, (DH, width), 0)).astype(BF16)
        filled = jnp.dot(stacked.astype(BF16), pick, preferred_element_type=F32)
        expand_ref[...] = jnp.where(
            same_head(filled.shape, slices, DH), filled, 0.0
        ).astype(BF16)
        own = same_head((columns, heads), slices, 1)
        sharp = jnp.sum(jnp.where(own, sharp_row_ref[...], 0.0), axis=1, keepdims=True)
        scale_ref[...] = LOG2E / sharp
        row = lax.broadcasted_iota(jnp.int32, (columns, slices), 0) % slices
        match = row == lax.broadcasted_iota(jnp.int32, (columns, slices), 1)
        offset_ref[...] = jnp.sum(
            jnp.where(match, offset_row_ref[...], 0.0), axis=1, keepdims=True
        )

    normed = norm_rows(x_ref[...].astype(F32), gain_ref[...], bias_ref[...])
    both = lax.dot_general(w_ref[...], normed, NT, preferred_element_type=F32).astype(BF16)
    share = slice_weights(
        both[width:], expand_ref[...], offset_ref[...], scale_ref[...], slices
    )
    numer[...] += lax.dot_general(
        both[:width], share.astype(BF16), NT, preferred_element_type=F32
    )
    lanes = total.shape[1]
    part = share[:, :lanes]
    for at in range(lanes, share.shape[1], lanes):
        part += share[:, at : at + lanes]
    total[...] += part

    @pl.when(step == pl.num_programs(0) - 1)
    def _():
        kept = jnp.where(same_head(numer.shape, DH, slices), numer[...], 0.0)
        out_ref[:DH] = jnp.sum(kept.reshape(-1, DH, kept.shape[1]), axis=0)
        out_ref[DH:] = lax.dot_general(
            jnp.ones((8, lanes), F32), total[...], NT, precision=HIGHEST,
            preferred_element_type=F32,
        )


def exact_gelu(h):
    half = 0.5 * h
    return half + half * lax.erf(h * (1.0 / math.sqrt(2.0)))


def blend_kernel(slices, sums_ref, question_ref, lookup_ref, content_ref, blend):
    stok = sums_ref[:DH] / (sums_ref[DH : DH + 1] + 1e-05)
    query, key, value = (
        jnp.dot(m[...].T, stok, precision=HIGHEST, preferred_element_type=F32)
        for m in (question_ref, lookup_ref, content_ref)
    )
    scores = jnp.dot(key.T, query, precision=HIGHEST, preferred_element_type=F32)
    scores = scores * (1.0 / math.sqrt(DH))
    mask = same_head(scores.shape, slices, slices)
    scores = jnp.where(mask, scores, -jnp.inf)
    powers = jnp.exp(scores - jnp.max(scores, axis=0, keepdims=True))
    attention = powers / jnp.sum(powers, axis=0, keepdims=True)
    sout = jnp.dot(value, attention, precision=HIGHEST, preferred_element_type=F32)
    spread = jnp.concatenate([sout] * (blend.shape[0] // DH), axis=0)
    blend[...] = jnp.where(same_head(blend.shape, DH, slices), spread, 0.0).astype(BF16)


def rows_kernel(
    slices, x_ref, blend, gain_ref, bias_ref, w_ref, expand_ref, offset_ref,
    scale_ref, emit_ref, emit_bias_ref, gain2_ref, bias2_ref, entry_ref, entry_bias_ref,
    exit_ref, exit_bias_ref, *earlier_and_out,
):
    out_ref = earlier_and_out[-1]
    width = x_ref.shape[1]
    x = x_ref[...].astype(F32)
    normed = norm_rows(x, gain_ref[...], bias_ref[...])
    feeder = lax.dot_general(w_ref[width:], normed, NT, preferred_element_type=F32).astype(BF16)
    share = slice_weights(feeder, expand_ref[...], offset_ref[...], scale_ref[...], slices)
    mixed = jnp.dot(blend[...], share.astype(BF16), preferred_element_type=F32)
    y = (
        x
        + jnp.dot(mixed.T.astype(BF16), emit_ref[...], preferred_element_type=F32)
        + emit_bias_ref[...]
    )
    z = norm_rows(y, gain2_ref[...], bias2_ref[...])
    result = y + exit_bias_ref[...]
    chunk = x_ref.shape[1]
    for at in range(0, entry_ref.shape[1], chunk):
        h = jnp.dot(z, entry_ref[:, at : at + chunk], preferred_element_type=F32)
        g = exact_gelu(h + entry_bias_ref[:, at : at + chunk]).astype(BF16)
        result += jnp.dot(g, exit_ref[at : at + chunk], preferred_element_type=F32)
    out_ref[...] = result.astype(BF16)


def whole(array):
    return pl.BlockSpec(array.shape, lambda i: (0,) * array.ndim)


def body(
    layer_inputs_trainorder,
    inference_placement,
    initial_layernorm_gain,
    initial_layernorm_offset,
    attribute_projection,
    assignment_feeder_projection,
    partition_projection,
    partition_offset,
    softmax_sharpness,
    partition_question_map,
    partition_lookup_map,
    partition_content_map,
    emitted_projection,
    emitted_offset,
    latter_layernorm_gain,
    latter_layernorm_offset,
    perceptron_entry_map,
    perceptron_entry_offset,
    perceptron_exit_map,
    perceptron_exit_offset,
):
    groups = lax.axis_size("head")
    shards = lax.axis_size("pts")
    devices = groups * shards
    both = ("head", "pts")
    local_rows, width = layer_inputs_trainorder.shape
    per_pair = local_rows // devices
    own_heads = softmax_sharpness.shape[0]
    heads = own_heads * groups
    slices = partition_projection.shape[1]
    columns = heads * slices
    chunk_pair = per_pair // CHUNKS
    chunk_rows = chunk_pair * devices
    tile = math.gcd(TILE, chunk_rows)

    sharpness = lax.all_to_all(
        jnp.broadcast_to(softmax_sharpness, (groups, own_heads)), "head", split_axis=0,
        concat_axis=0, tiled=True,
    ).reshape(1, heads)

    dest_block = inference_placement // local_rows
    target = dest_block % groups * shards + dest_block // groups
    send_key = target * local_rows + inference_placement % local_rows
    counting = jnp.arange(local_rows, dtype=jnp.int32)
    send_key, ordering = lax.sort((send_key, counting), num_keys=1)
    ordering = ordering.reshape(devices, CHUNKS, chunk_pair)
    spots = (send_key % local_rows).reshape(devices, per_pair)

    def gathered(order):
        return layer_inputs_trainorder[order.reshape(chunk_rows)]

    def exchange(rows):
        return lax.all_to_all(rows, both, split_axis=0, concat_axis=0, tiled=True)

    arrived = [exchange(gathered(ordering[:, 0]))]
    arrived_spots = exchange(spots).reshape(devices, CHUNKS, chunk_pair)
    arrived_spots = arrived_spots.transpose(1, 0, 2).reshape(local_rows)
    _, placed = lax.sort((arrived_spots, counting), num_keys=1)

    gain = initial_layernorm_gain[None]
    bias = initial_layernorm_offset[None]
    operands = (
        gain, bias, attribute_projection, assignment_feeder_projection, partition_projection,
        partition_offset[None], sharpness,
    )
    made = (
        jax.ShapeDtypeStruct((DH + 8, columns), F32),
        jax.ShapeDtypeStruct((2 * width, width), BF16),
        jax.ShapeDtypeStruct((columns, width), BF16),
        jax.ShapeDtypeStruct((columns, 1), F32),
        jax.ShapeDtypeStruct((columns, 1), F32),
    )
    sums, *constants = pl.pallas_call(
        functools.partial(sums_kernel, slices),
        grid=(local_rows // tile,),
        in_specs=[pl.BlockSpec((tile, width), lambda i: (i, 0))] + [whole(a) for a in operands],
        out_specs=[whole(a) for a in made],
        out_shape=made,
        scratch_shapes=[pltpu.VMEM((width, columns), F32), pltpu.VMEM((columns, 128), F32)],
        compiler_params=pltpu.CompilerParams(dimension_semantics=("arbitrary",)),
        cost_estimate=pl.CostEstimate(
            flops=local_rows * width * columns * 8, bytes_accessed=local_rows * width * 16,
            transcendentals=local_rows * columns,
        ),
    )(layer_inputs_trainorder, *operands)

    waiting, sums = lax.optimization_barrier((gathered(ordering[:, 1]), sums))
    sums = lax.psum(sums, both)
    waiting, later, sums = lax.optimization_barrier((waiting, ordering[:, 2:], sums))
    arrived.append(exchange(waiting))
    for at in range(CHUNKS - 2):
        arrived.append(exchange(gathered(later[:, at])))

    maps = (sums, partition_question_map, partition_lookup_map, partition_content_map)
    blend = pl.pallas_call(
        functools.partial(blend_kernel, slices),
        out_shape=jax.ShapeDtypeStruct((width, columns), BF16),
        cost_estimate=pl.CostEstimate(
            flops=columns * columns * 1000, bytes_accessed=columns * width * 8,
            transcendentals=columns * columns,
        ),
    )(*maps)

    operands = (
        blend, gain, bias, *constants, emitted_projection,
        emitted_offset[None], latter_layernorm_gain[None], latter_layernorm_offset[None],
        perceptron_entry_map, perceptron_entry_offset[None], perceptron_exit_map,
        perceptron_exit_offset[None],
    )
    result = ()
    steps = chunk_rows // tile
    for at in range(CHUNKS):
        result = pl.pallas_call(
            functools.partial(rows_kernel, slices),
            grid=(steps,),
            in_specs=[pl.BlockSpec((tile, width), lambda i: (i, 0))]
            + [whole(a) for a in operands]
            + [pl.BlockSpec(memory_space=pl.ANY) for _ in result],
            out_specs=(pl.BlockSpec((tile, width), lambda i, at=at: (i + at * steps, 0)),),
            out_shape=(jax.ShapeDtypeStruct((local_rows, width), BF16),),
            input_output_aliases={1 + len(operands): 0} if result else {},
            compiler_params=pltpu.CompilerParams(dimension_semantics=("arbitrary",)),
            cost_estimate=pl.CostEstimate(
                flops=chunk_rows * width * columns * 16, bytes_accessed=chunk_rows * width * 16,
                transcendentals=chunk_rows * columns * 4,
            ),
        )(arrived[at], *operands, *result)
    return result[0][placed][None]


def solution(mesh):
    placed = (
        P(("head", "pts"), None),
        P(("head", "pts")),
        P(),
        P(),
        P(),
        P(),
        P(),
        P(),
        P("head"),
        P(),
        P(),
        P(),
        P(),
        P(),
        P(),
        P(),
        P(),
        P(),
        P(),
        P(),
    )
    return jax.shard_map(
        body, mesh=mesh, in_specs=placed, out_specs=P("pts", "head", None), check_vma=False
    )
```

```python
import functools
import math

import jax
import jax.numpy as jnp
from jax import lax
from jax.experimental import pallas as pl
from jax.experimental.pallas import tpu as pltpu
from jax.sharding import PartitionSpec as P

DH = 16
TILE = 512
CHUNKS = 3
F32 = jnp.float32
BF16 = jnp.bfloat16
HIGHEST = lax.Precision.HIGHEST
LOG2E = math.log2(math.e)
NT = (((1,), (1,)), ((), ()))


def norm_rows(rows, gain, bias):
    mean = jnp.mean(rows, axis=-1, keepdims=True)
    centred = rows - mean
    spread = jnp.mean(centred * centred, axis=-1, keepdims=True)
    return (centred * lax.rsqrt(spread + 1e-05) * gain + bias).astype(BF16)


def slice_weights(feeder_t, expand, offset, scale, slices):
    raw = jnp.dot(expand, feeder_t, preferred_element_type=F32)
    logit = (raw + offset) * scale
    lanes = logit.shape[1]
    logit = logit.reshape(-1, slices, lanes)
    powers = jnp.exp2(logit - jnp.max(logit, axis=1, keepdims=True))
    share = powers * (1.0 / jnp.sum(powers, axis=1, keepdims=True))
    return share.reshape(-1, lanes)


def same_head(shape, row_size, column_size):
    row_head = lax.broadcasted_iota(jnp.int32, shape, 0) // row_size
    column_head = lax.broadcasted_iota(jnp.int32, shape, 1) // column_size
    return row_head == column_head


def sums_kernel(
    slices, x_ref, gain_ref, bias_ref, attribute_ref, feeder_ref, project_ref, offset_row_ref,
    sharp_row_ref, out_ref, w_ref, expand_ref, offset_ref, scale_ref, numer, total,
):
    step = pl.program_id(0)
    width = x_ref.shape[1]

    @pl.when(step == 0)
    def _():
        numer[...] = jnp.zeros_like(numer)
        total[...] = jnp.zeros_like(total)
        w_ref[:width] = attribute_ref[...].astype(F32).T.astype(BF16)
        w_ref[width:] = feeder_ref[...].astype(F32).T.astype(BF16)
        columns, heads = offset_ref.shape[0], sharp_row_ref.shape[1]
        stacked = jnp.concatenate([project_ref[...].astype(F32).T] * heads, axis=0)
        lane = lax.broadcasted_iota(jnp.int32, (DH, width), 1) % DH
        pick = (lane == lax.broadcasted_iota(jnp.int32, (DH, width), 0)).astype(BF16)
        filled = jnp.dot(stacked.astype(BF16), pick, preferred_element_type=F32)
        expand_ref[...] = jnp.where(
            same_head(filled.shape, slices, DH), filled, 0.0
        ).astype(BF16)
        own = same_head((columns, heads), slices, 1)
        sharp = jnp.sum(jnp.where(own, sharp_row_ref[...], 0.0), axis=1, keepdims=True)
        scale_ref[...] = LOG2E / sharp
        row = lax.broadcasted_iota(jnp.int32, (columns, slices), 0) % slices
        match = row == lax.broadcasted_iota(jnp.int32, (columns, slices), 1)
        offset_ref[...] = jnp.sum(
            jnp.where(match, offset_row_ref[...], 0.0), axis=1, keepdims=True
        )

    normed = norm_rows(x_ref[...].astype(F32), gain_ref[...], bias_ref[...])
    both = lax.dot_general(w_ref[...], normed, NT, preferred_element_type=F32).astype(BF16)
    share = slice_weights(
        both[width:], expand_ref[...], offset_ref[...], scale_ref[...], slices
    )
    numer[...] += lax.dot_general(
        both[:width], share.astype(BF16), NT, preferred_element_type=F32
    )
    lanes = total.shape[1]
    part = share[:, :lanes]
    for at in range(lanes, share.shape[1], lanes):
        part += share[:, at : at + lanes]
    total[...] += part

    @pl.when(step == pl.num_programs(0) - 1)
    def _():
        kept = jnp.where(same_head(numer.shape, DH, slices), numer[...], 0.0)
        out_ref[:DH] = jnp.sum(kept.reshape(-1, DH, kept.shape[1]), axis=0)
        out_ref[DH:] = lax.dot_general(
            jnp.ones((8, lanes), F32), total[...], NT, precision=HIGHEST,
            preferred_element_type=F32,
        )


def exact_gelu(h):
    half = 0.5 * h
    return half + half * lax.erf(h * (1.0 / math.sqrt(2.0)))


def blend_kernel(slices, sums_ref, question_ref, lookup_ref, content_ref, blend):
    stok = sums_ref[:DH] / (sums_ref[DH : DH + 1] + 1e-05)
    query, key, value = (
        jnp.dot(m[...].T, stok, precision=HIGHEST, preferred_element_type=F32)
        for m in (question_ref, lookup_ref, content_ref)
    )
    scores = jnp.dot(key.T, query, precision=HIGHEST, preferred_element_type=F32)
    scores = scores * (1.0 / math.sqrt(DH))
    mask = same_head(scores.shape, slices, slices)
    scores = jnp.where(mask, scores, -jnp.inf)
    powers = jnp.exp(scores - jnp.max(scores, axis=0, keepdims=True))
    attention = powers / jnp.sum(powers, axis=0, keepdims=True)
    sout = jnp.dot(value, attention, precision=HIGHEST, preferred_element_type=F32)
    spread = jnp.concatenate([sout] * (blend.shape[0] // DH), axis=0)
    blend[...] = jnp.where(same_head(blend.shape, DH, slices), spread, 0.0).astype(BF16)


def rows_kernel(
    slices, x_ref, blend, gain_ref, bias_ref, w_ref, expand_ref, offset_ref,
    scale_ref, emit_ref, emit_bias_ref, gain2_ref, bias2_ref, entry_ref, entry_bias_ref,
    exit_ref, exit_bias_ref, *earlier_and_out,
):
    out_ref = earlier_and_out[-1]
    width = x_ref.shape[1]
    x = x_ref[...].astype(F32)
    normed = norm_rows(x, gain_ref[...], bias_ref[...])
    feeder = lax.dot_general(w_ref[width:], normed, NT, preferred_element_type=F32).astype(BF16)
    share = slice_weights(feeder, expand_ref[...], offset_ref[...], scale_ref[...], slices)
    mixed = jnp.dot(blend[...], share.astype(BF16), preferred_element_type=F32)
    y = (
        x
        + jnp.dot(mixed.T.astype(BF16), emit_ref[...], preferred_element_type=F32)
        + emit_bias_ref[...]
    )
    z = norm_rows(y, gain2_ref[...], bias2_ref[...])
    result = y + exit_bias_ref[...]
    chunk = x_ref.shape[1]
    for at in range(0, entry_ref.shape[1], chunk):
        h = jnp.dot(z, entry_ref[:, at : at + chunk], preferred_element_type=F32)
        g = exact_gelu(h + entry_bias_ref[:, at : at + chunk]).astype(BF16)
        result += jnp.dot(g, exit_ref[at : at + chunk], preferred_element_type=F32)
    out_ref[...] = result.astype(BF16)


def whole(array):
    return pl.BlockSpec(array.shape, lambda i: (0,) * array.ndim)


def body(
    layer_inputs_trainorder,
    inference_placement,
    initial_layernorm_gain,
    initial_layernorm_offset,
    attribute_projection,
    assignment_feeder_projection,
    partition_projection,
    partition_offset,
    softmax_sharpness,
    partition_question_map,
    partition_lookup_map,
    partition_content_map,
    emitted_projection,
    emitted_offset,
    latter_layernorm_gain,
    latter_layernorm_offset,
    perceptron_entry_map,
    perceptron_entry_offset,
    perceptron_exit_map,
    perceptron_exit_offset,
):
    groups = lax.axis_size("head")
    shards = lax.axis_size("pts")
    devices = groups * shards
    both = ("head", "pts")
    local_rows, width = layer_inputs_trainorder.shape
    per_pair = local_rows // devices
    own_heads = softmax_sharpness.shape[0]
    heads = own_heads * groups
    slices = partition_projection.shape[1]
    columns = heads * slices
    chunk_pair = per_pair // CHUNKS
    chunk_rows = chunk_pair * devices
    tile = math.gcd(TILE, chunk_rows)

    dest_block = inference_placement // local_rows
    target = dest_block % groups * shards + dest_block // groups
    send_key = target * local_rows + inference_placement % local_rows
    counting = jnp.arange(local_rows, dtype=jnp.int32)
    send_key, ordering = lax.sort((send_key, counting), num_keys=1)
    ordering = ordering.reshape(devices, CHUNKS, chunk_pair)
    spots = (send_key % local_rows).astype(F32).reshape(devices, per_pair)
    small = jnp.concatenate(
        [spots, jnp.broadcast_to(softmax_sharpness, (devices, own_heads))], axis=1
    )

    def gathered(order):
        return layer_inputs_trainorder[order.reshape(chunk_rows)]

    def exchange(rows):
        return lax.all_to_all(rows, both, split_axis=0, concat_axis=0, tiled=True)

    arrived = [exchange(gathered(ordering[:, 0]))]
    small = exchange(small)
    sharpness = small.reshape(groups, shards, -1)[:, 0, per_pair:].reshape(1, heads)
    arrived_spots = small[:, :per_pair].astype(jnp.int32).reshape(devices, CHUNKS, chunk_pair)
    arrived_spots = arrived_spots.transpose(1, 0, 2).reshape(local_rows)
    _, placed = lax.sort((arrived_spots, counting), num_keys=1)

    gain = initial_layernorm_gain[None]
    bias = initial_layernorm_offset[None]
    operands = (
        gain, bias, attribute_projection, assignment_feeder_projection, partition_projection,
        partition_offset[None], sharpness,
    )
    made = (
        jax.ShapeDtypeStruct((DH + 8, columns), F32),
        jax.ShapeDtypeStruct((2 * width, width), BF16),
        jax.ShapeDtypeStruct((columns, width), BF16),
        jax.ShapeDtypeStruct((columns, 1), F32),
        jax.ShapeDtypeStruct((columns, 1), F32),
    )
    sums, *constants = pl.pallas_call(
        functools.partial(sums_kernel, slices),
        grid=(local_rows // tile,),
        in_specs=[pl.BlockSpec((tile, width), lambda i: (i, 0))] + [whole(a) for a in operands],
        out_specs=[whole(a) for a in made],
        out_shape=made,
        scratch_shapes=[pltpu.VMEM((width, columns), F32), pltpu.VMEM((columns, 128), F32)],
        compiler_params=pltpu.CompilerParams(dimension_semantics=("arbitrary",)),
        cost_estimate=pl.CostEstimate(
            flops=local_rows * width * columns * 8, bytes_accessed=local_rows * width * 16,
            transcendentals=local_rows * columns,
        ),
    )(layer_inputs_trainorder, *operands)

    waiting, sums, arrived[0] = lax.optimization_barrier(
        (gathered(ordering[:, 1]), sums, arrived[0])
    )
    part = jnp.sum(exchange(sums.reshape(devices, -1)), axis=0)
    sums = exchange(jnp.broadcast_to(part, (devices,) + part.shape)).reshape(sums.shape)
    waiting, later, sums = lax.optimization_barrier((waiting, ordering[:, 2:], sums))
    arrived.append(exchange(waiting))
    later = [gathered(later[:, at]) for at in range(CHUNKS - 2)]

    maps = (sums, partition_question_map, partition_lookup_map, partition_content_map)
    blend = pl.pallas_call(
        functools.partial(blend_kernel, slices),
        out_shape=jax.ShapeDtypeStruct((width, columns), BF16),
        cost_estimate=pl.CostEstimate(
            flops=columns * columns * 1000, bytes_accessed=columns * width * 8,
            transcendentals=columns * columns,
        ),
    )(*maps)

    operands = (
        blend, gain, bias, *constants, emitted_projection,
        emitted_offset[None], latter_layernorm_gain[None], latter_layernorm_offset[None],
        perceptron_entry_map, perceptron_entry_offset[None], perceptron_exit_map,
        perceptron_exit_offset[None],
    )
    result = ()
    steps = chunk_rows // tile
    for at in range(CHUNKS):
        result = pl.pallas_call(
            functools.partial(rows_kernel, slices),
            grid=(steps,),
            in_specs=[pl.BlockSpec((tile, width), lambda i: (i, 0))]
            + [whole(a) for a in operands]
            + [pl.BlockSpec(memory_space=pl.ANY) for _ in result],
            out_specs=(pl.BlockSpec((tile, width), lambda i, at=at: (i + at * steps, 0)),),
            out_shape=(jax.ShapeDtypeStruct((local_rows, width), BF16),),
            input_output_aliases={1 + len(operands): 0} if result else {},
            compiler_params=pltpu.CompilerParams(dimension_semantics=("arbitrary",)),
            cost_estimate=pl.CostEstimate(
                flops=chunk_rows * width * columns * 16, bytes_accessed=chunk_rows * width * 16,
                transcendentals=chunk_rows * columns * 4,
            ),
        )(arrived[at], *operands, *result)
        if at + 2 < CHUNKS:
            leaving, result = lax.optimization_barrier((later[at], result))
            arrived.append(exchange(leaving))
    return result[0][placed][None]


def solution(mesh):
    placed = (
        P(("head", "pts"), None),
        P(("head", "pts")),
        P(),
        P(),
        P(),
        P(),
        P(),
        P(),
        P("head"),
        P(),
        P(),
        P(),
        P(),
        P(),
        P(),
        P(),
        P(),
        P(),
        P(),
        P(),
    )
    return jax.shard_map(
        body, mesh=mesh, in_specs=placed, out_specs=P("pts", "head", None), check_vma=False
    )
```

```python
import functools
import math

import jax
import jax.numpy as jnp
from jax import lax
from jax.experimental import pallas as pl
from jax.experimental.pallas import tpu as pltpu
from jax.sharding import PartitionSpec as P

DH = 16
TILE = 512
SHARES = (5, 4, 3)
F32 = jnp.float32
BF16 = jnp.bfloat16
HIGHEST = lax.Precision.HIGHEST
LOG2E = math.log2(math.e)
NT = (((1,), (1,)), ((), ()))


def norm_rows(rows, gain, bias):
    mean = jnp.mean(rows, axis=-1, keepdims=True)
    centred = rows - mean
    spread = jnp.mean(centred * centred, axis=-1, keepdims=True)
    return (centred * lax.rsqrt(spread + 1e-05) * gain + bias).astype(BF16)


def slice_weights(feeder_t, expand, offset, scale, slices):
    raw = jnp.dot(expand, feeder_t, preferred_element_type=F32)
    logit = (raw + offset) * scale
    lanes = logit.shape[1]
    logit = logit.reshape(-1, slices, lanes)
    powers = jnp.exp2(logit - jnp.max(logit, axis=1, keepdims=True))
    share = powers * (1.0 / jnp.sum(powers, axis=1, keepdims=True))
    return share.reshape(-1, lanes)


def same_head(shape, row_size, column_size):
    row_head = lax.broadcasted_iota(jnp.int32, shape, 0) // row_size
    column_head = lax.broadcasted_iota(jnp.int32, shape, 1) // column_size
    return row_head == column_head


def sums_kernel(
    slices, x_ref, gain_ref, bias_ref, attribute_ref, feeder_ref, project_ref, offset_row_ref,
    sharp_row_ref, out_ref, w_ref, expand_ref, offset_ref, scale_ref, numer, total,
):
    step = pl.program_id(0)
    width = x_ref.shape[1]

    @pl.when(step == 0)
    def _():
        numer[...] = jnp.zeros_like(numer)
        total[...] = jnp.zeros_like(total)
        w_ref[:width] = attribute_ref[...].astype(F32).T.astype(BF16)
        w_ref[width:] = feeder_ref[...].astype(F32).T.astype(BF16)
        columns, heads = offset_ref.shape[0], sharp_row_ref.shape[1]
        stacked = jnp.concatenate([project_ref[...].astype(F32).T] * heads, axis=0)
        lane = lax.broadcasted_iota(jnp.int32, (DH, width), 1) % DH
        pick = (lane == lax.broadcasted_iota(jnp.int32, (DH, width), 0)).astype(BF16)
        filled = jnp.dot(stacked.astype(BF16), pick, preferred_element_type=F32)
        expand_ref[...] = jnp.where(
            same_head(filled.shape, slices, DH), filled, 0.0
        ).astype(BF16)
        own = same_head((columns, heads), slices, 1)
        sharp = jnp.sum(jnp.where(own, sharp_row_ref[...], 0.0), axis=1, keepdims=True)
        scale_ref[...] = LOG2E / sharp
        row = lax.broadcasted_iota(jnp.int32, (columns, slices), 0) % slices
        match = row == lax.broadcasted_iota(jnp.int32, (columns, slices), 1)
        offset_ref[...] = jnp.sum(
            jnp.where(match, offset_row_ref[...], 0.0), axis=1, keepdims=True
        )

    normed = norm_rows(x_ref[...].astype(F32), gain_ref[...], bias_ref[...])
    both = lax.dot_general(w_ref[...], normed, NT, preferred_element_type=F32).astype(BF16)
    share = slice_weights(
        both[width:], expand_ref[...], offset_ref[...], scale_ref[...], slices
    )
    numer[...] += lax.dot_general(
        both[:width], share.astype(BF16), NT, preferred_element_type=F32
    )
    lanes = total.shape[1]
    part = share[:, :lanes]
    for at in range(lanes, share.shape[1], lanes):
        part += share[:, at : at + lanes]
    total[...] += part

    @pl.when(step == pl.num_programs(0) - 1)
    def _():
        kept = jnp.where(same_head(numer.shape, DH, slices), numer[...], 0.0)
        out_ref[:DH] = jnp.sum(kept.reshape(-1, DH, kept.shape[1]), axis=0)
        out_ref[DH:] = lax.dot_general(
            jnp.ones((8, lanes), F32), total[...], NT, precision=HIGHEST,
            preferred_element_type=F32,
        )


def exact_gelu(h):
    half = 0.5 * h
    return half + half * lax.erf(h * (1.0 / math.sqrt(2.0)))


def blend_kernel(slices, sums_ref, question_ref, lookup_ref, content_ref, blend):
    stok = sums_ref[:DH] / (sums_ref[DH : DH + 1] + 1e-05)
    query, key, value = (
        jnp.dot(m[...].T, stok, precision=HIGHEST, preferred_element_type=F32)
        for m in (question_ref, lookup_ref, content_ref)
    )
    scores = jnp.dot(key.T, query, precision=HIGHEST, preferred_element_type=F32)
    scores = scores * (1.0 / math.sqrt(DH))
    mask = same_head(scores.shape, slices, slices)
    scores = jnp.where(mask, scores, -jnp.inf)
    powers = jnp.exp(scores - jnp.max(scores, axis=0, keepdims=True))
    attention = powers / jnp.sum(powers, axis=0, keepdims=True)
    sout = jnp.dot(value, attention, precision=HIGHEST, preferred_element_type=F32)
    spread = jnp.concatenate([sout] * (blend.shape[0] // DH), axis=0)
    blend[...] = jnp.where(same_head(blend.shape, DH, slices), spread, 0.0).astype(BF16)


def rows_kernel(
    slices, x_ref, blend, gain_ref, bias_ref, w_ref, expand_ref, offset_ref,
    scale_ref, emit_ref, emit_bias_ref, gain2_ref, bias2_ref, entry_ref, entry_bias_ref,
    exit_ref, exit_bias_ref, *earlier_and_out,
):
    out_ref = earlier_and_out[-1]
    width = x_ref.shape[1]
    x = x_ref[...].astype(F32)
    normed = norm_rows(x, gain_ref[...], bias_ref[...])
    feeder = lax.dot_general(w_ref[width:], normed, NT, preferred_element_type=F32).astype(BF16)
    share = slice_weights(feeder, expand_ref[...], offset_ref[...], scale_ref[...], slices)
    mixed = jnp.dot(blend[...], share.astype(BF16), preferred_element_type=F32)
    y = (
        x
        + jnp.dot(mixed.T.astype(BF16), emit_ref[...], preferred_element_type=F32)
        + emit_bias_ref[...]
    )
    z = norm_rows(y, gain2_ref[...], bias2_ref[...])
    result = y + exit_bias_ref[...]
    chunk = x_ref.shape[1]
    for at in range(0, entry_ref.shape[1], chunk):
        h = jnp.dot(z, entry_ref[:, at : at + chunk], preferred_element_type=F32)
        g = exact_gelu(h + entry_bias_ref[:, at : at + chunk]).astype(BF16)
        result += jnp.dot(g, exit_ref[at : at + chunk], preferred_element_type=F32)
    out_ref[...] = result.astype(BF16)


def whole(array):
    return pl.BlockSpec(array.shape, lambda i: (0,) * array.ndim)


def body(
    layer_inputs_trainorder,
    inference_placement,
    initial_layernorm_gain,
    initial_layernorm_offset,
    attribute_projection,
    assignment_feeder_projection,
    partition_projection,
    partition_offset,
    softmax_sharpness,
    partition_question_map,
    partition_lookup_map,
    partition_content_map,
    emitted_projection,
    emitted_offset,
    latter_layernorm_gain,
    latter_layernorm_offset,
    perceptron_entry_map,
    perceptron_entry_offset,
    perceptron_exit_map,
    perceptron_exit_offset,
):
    groups = lax.axis_size("head")
    shards = lax.axis_size("pts")
    devices = groups * shards
    both = ("head", "pts")
    local_rows, width = layer_inputs_trainorder.shape
    per_pair = local_rows // devices
    own_heads = softmax_sharpness.shape[0]
    heads = own_heads * groups
    slices = partition_projection.shape[1]
    columns = heads * slices
    unit = per_pair // sum(SHARES)
    ends = [unit * sum(SHARES[: at + 1]) for at in range(len(SHARES))]
    spans = list(zip([0] + ends[:-1], ends))
    tile = math.gcd(TILE, *(high * devices for high in ends))

    dest_block = inference_placement // local_rows
    target = dest_block % groups * shards + dest_block // groups
    send_key = target * local_rows + inference_placement % local_rows
    counting = jnp.arange(local_rows, dtype=jnp.int32)
    send_key, ordering = lax.sort((send_key, counting), num_keys=1)
    ordering = ordering.reshape(devices, per_pair)
    spots = (send_key % local_rows).astype(F32).reshape(devices, per_pair)
    small = jnp.concatenate(
        [spots, jnp.broadcast_to(softmax_sharpness, (devices, own_heads))], axis=1
    )

    def gathered(order):
        return layer_inputs_trainorder[order.reshape(-1)]

    def exchange(rows):
        return lax.all_to_all(rows, both, split_axis=0, concat_axis=0, tiled=True)

    arrived = [exchange(gathered(ordering[:, : ends[0]]))]
    small = exchange(small)
    sharpness = small.reshape(groups, shards, -1)[:, 0, per_pair:].reshape(1, heads)
    arrived_spots = small[:, :per_pair].astype(jnp.int32)
    arrived_spots = jnp.concatenate(
        [arrived_spots[:, low:high].reshape(-1) for low, high in spans]
    )
    _, placed = lax.sort((arrived_spots, counting), num_keys=1)

    gain = initial_layernorm_gain[None]
    bias = initial_layernorm_offset[None]
    operands = (
        gain, bias, attribute_projection, assignment_feeder_projection, partition_projection,
        partition_offset[None], sharpness,
    )
    made = (
        jax.ShapeDtypeStruct((DH + 8, columns), F32),
        jax.ShapeDtypeStruct((2 * width, width), BF16),
        jax.ShapeDtypeStruct((columns, width), BF16),
        jax.ShapeDtypeStruct((columns, 1), F32),
        jax.ShapeDtypeStruct((columns, 1), F32),
    )
    sums, *constants = pl.pallas_call(
        functools.partial(sums_kernel, slices),
        grid=(local_rows // tile,),
        in_specs=[pl.BlockSpec((tile, width), lambda i: (i, 0))] + [whole(a) for a in operands],
        out_specs=[whole(a) for a in made],
        out_shape=made,
        scratch_shapes=[pltpu.VMEM((width, columns), F32), pltpu.VMEM((columns, 128), F32)],
        compiler_params=pltpu.CompilerParams(dimension_semantics=("arbitrary",)),
        cost_estimate=pl.CostEstimate(
            flops=local_rows * width * columns * 8, bytes_accessed=local_rows * width * 16,
            transcendentals=local_rows * columns,
        ),
    )(layer_inputs_trainorder, *operands)

    waiting, sums, arrived[0] = lax.optimization_barrier(
        (gathered(ordering[:, ends[0] : ends[1]]), sums, arrived[0])
    )
    part = jnp.sum(exchange(sums.reshape(devices, -1)), axis=0)
    sums = exchange(jnp.broadcast_to(part, (devices,) + part.shape)).reshape(sums.shape)
    waiting, later, sums = lax.optimization_barrier((waiting, ordering, sums))
    arrived.append(exchange(waiting))
    later = [gathered(later[:, low:high]) for low, high in spans[2:]]

    maps = (sums, partition_question_map, partition_lookup_map, partition_content_map)
    blend = pl.pallas_call(
        functools.partial(blend_kernel, slices),
        out_shape=jax.ShapeDtypeStruct((width, columns), BF16),
        cost_estimate=pl.CostEstimate(
            flops=columns * columns * 1000, bytes_accessed=columns * width * 8,
            transcendentals=columns * columns,
        ),
    )(*maps)

    operands = (
        blend, gain, bias, *constants, emitted_projection,
        emitted_offset[None], latter_layernorm_gain[None], latter_layernorm_offset[None],
        perceptron_entry_map, perceptron_entry_offset[None], perceptron_exit_map,
        perceptron_exit_offset[None],
    )
    result = ()
    for at, (low, high) in enumerate(spans):
        chunk_rows = (high - low) * devices
        first = low * devices // tile
        result = pl.pallas_call(
            functools.partial(rows_kernel, slices),
            grid=(chunk_rows // tile,),
            in_specs=[pl.BlockSpec((tile, width), lambda i: (i, 0))]
            + [whole(a) for a in operands]
            + [pl.BlockSpec(memory_space=pl.ANY) for _ in result],
            out_specs=(pl.BlockSpec((tile, width), lambda i, first=first: (i + first, 0)),),
            out_shape=(jax.ShapeDtypeStruct((local_rows, width), BF16),),
            input_output_aliases={1 + len(operands): 0} if result else {},
            compiler_params=pltpu.CompilerParams(dimension_semantics=("arbitrary",)),
            cost_estimate=pl.CostEstimate(
                flops=chunk_rows * width * columns * 16, bytes_accessed=chunk_rows * width * 16,
                transcendentals=chunk_rows * columns * 4,
            ),
        )(arrived[at], *operands, *result)
        if at + 2 < len(SHARES):
            leaving, result = lax.optimization_barrier((later[at], result))
            arrived.append(exchange(leaving))
    return result[0][placed][None]


def solution(mesh):
    placed = (
        P(("head", "pts"), None),
        P(("head", "pts")),
        P(),
        P(),
        P(),
        P(),
        P(),
        P(),
        P("head"),
        P(),
        P(),
        P(),
        P(),
        P(),
        P(),
        P(),
        P(),
        P(),
        P(),
        P(),
    )
    return jax.shard_map(
        body, mesh=mesh, in_specs=placed, out_specs=P("pts", "head", None), check_vma=False
    )
```
